128 devices in a mesh: band: 32 (over y, x, core), lev: 4 (over z).
Axes of the slice: x: 4, y: 4, z: 4, core: 2. Of those that a mesh axis runs over, the one named last changes fastest.
Arguments:
- increment: bfloat16 [32, 768, 1536], P('lev', 'band'), may hold values from -6 to 6
- background: float32 [384, 2, 32, 769], P(('band', 'lev')), may hold values from -6 to 6
- legendre: bfloat16 [384, 768, 769], P(('band', 'lev')), may hold values from -6 to 6, as said below
- coupling: float32 [4, 32, 32], replicated, may hold values from -1 to 1
- damping: float32 [4], replicated, may hold values from 0.5 to 4
- target_mass: float32 [1], replicated, may hold values from 1 to 4
- numerators: int32 [4], replicated, may hold values from 8 to 32
- pair_low: int32 [384], replicated, may hold values from 0 to 383, as said below
- lat_map: int32 [768], replicated, may hold values from 0 to 767, each once
Outputs:
- analysis: bfloat16 [32, 768, 1536], P('lev', 'band')
- corrections: float32 [4], replicated
The draws below stay inside these ranges and needn't reach their ends.
Inputs may be any that keep to these rules, and one draw needn't show every extreme that they name: Slot p holds the wavenumbers pair_low[p] and 767 - pair_low[p]; every value appears once. For the slot p with pair_low[p] = 0, legendre[p, j, 0] = 1 at every latitude j. Stored grid row r lies on latitude lat_map[r]; every latitude appears once.
All inputs are finite; a program needn't handle non-finite values.
Results may differ from the reference program's by a relative error of at most 0.0078.
Values may be sent and summed in bfloat16 or wider, within the bound.
A program may use at most 128 MiB of HBM per device.

```python
import math
import jax
import jax.numpy as jnp
from jax import lax

NT = 767
NLAT = 768
NLON = 1536
LEV = 32
STEPS = 4
DEN = 64
NPAIR = 384


def pair_order(key):
    return jax.random.permutation(jax.random.fold_in(key, 7001), NPAIR).astype(jnp.int32)


def draw_pair_low(key, part):
    return pair_order(key)


def draw_legendre(key, part):
    pairs = pair_order(key)
    sub = jax.random.fold_in(key, 7002)
    scale_key = jax.random.fold_in(key, 7003)
    values = jax.random.truncated_normal(sub, -3.0, 3.0, (NPAIR, NLAT, NT + 2), jnp.float32)
    log_scale = jax.random.uniform(scale_key, (NLAT,), jnp.float32, jnp.log(0.5), jnp.log(2.0))
    values = values * jnp.exp(log_scale)[None, :, None]
    column = jnp.where(pairs[:, None] == 0, jnp.ones_like(values[:, :, 0]), values[:, :, 0])
    values = values.at[:, :, 0].set(column)
    return values.astype(jnp.bfloat16)


def place_ends(drawn, rng, smallest, high):
    longest = drawn.shape.index(max(drawn.shape))
    spots = []
    for shift in (0, 1):
        where = [jax.random.randint(jax.random.fold_in(rng, axis), (), 0, length) for axis, length in enumerate(drawn.shape)]
        where[longest] = (where[longest] + shift) % drawn.shape[longest]
        spots.append(tuple(where))
    return drawn.at[spots[0]].set(smallest).at[spots[1]].set(high)


def shard_levels(stream_key, dims, cuts, low, top_value):
    def one(dim, blocks):
        draws = jax.random.uniform(jax.random.fold_in(jax.random.fold_in(stream_key, 6), dim), (blocks,), jnp.float32, low / len(cuts), top_value / len(cuts))
        return jnp.repeat(jnp.exp(draws), dims[dim] // blocks).reshape((-1,) + (1,) * (len(dims) - dim - 1))

    level = one(*cuts[0])
    for cut in cuts[1:]:
        level = level * one(*cut)
    return level


def centred(rng, extent, width, reach, split=(), held_as=jnp.bfloat16):
    array = width * jax.random.normal(rng, extent, jnp.float32)
    if split:
        array = array * shard_levels(rng, extent, split, -0.22, 0.18)
    return jnp.clip(array, -reach, reach).astype(held_as)


def setup_inputs(seed: int = 0) -> dict:
    streams_of = jax.random.split(jax.random.key(seed), 10)
    return {
        "increment": centred(streams_of[0], (LEV, NLAT, NLON), 1.0, 6.0, ((0, 4), (1, 32))),
        "background": centred(streams_of[1], (NPAIR, 2, LEV, NT + 2), 1.0, 6.0, ((0, 128),), jnp.float32),
        "legendre": draw_legendre(jax.random.fold_in(streams_of[9], 71), 0),
        "coupling": centred(streams_of[3], (STEPS, LEV, LEV), LEV ** -0.5, 1.0, (), jnp.float32),
        "damping": jnp.clip(jnp.exp(jax.random.uniform(streams_of[4], (STEPS,), jnp.float32, math.log(0.5), math.log(4.0))), 0.5, 4.0),
        "target_mass": jnp.clip(jnp.exp(jax.random.uniform(streams_of[5], (1,), jnp.float32, math.log(1.0), math.log(4.0))), 1.0, 4.0),
        "numerators": place_ends(jax.random.randint(streams_of[6], (STEPS,), 8, 33), jax.random.fold_in(streams_of[6], 1), 8, 32).astype(jnp.int32),
        "pair_low": draw_pair_low(jax.random.fold_in(streams_of[9], 71), 0),
        "lat_map": jax.random.permutation(streams_of[8], NLAT).astype(jnp.int32),
    }


def wave_table(pair_low):
    member = jnp.arange(4, dtype=jnp.int32) // 2
    re_im = jnp.arange(4, dtype=jnp.int32) % 2
    wavenumber = jnp.where(member[None, :] == 0, pair_low[:, None], NT - pair_low[:, None]).reshape(-1)
    part_of = jnp.tile(re_im, pair_low.shape[0])
    points = jnp.arange(NLON, dtype=jnp.int32)
    phase_idx = wavenumber[:, None] * points[None, :] % NLON
    angles = phase_idx.astype(jnp.float32) * (2.0 * math.pi / NLON)
    values = jnp.where(part_of[:, None] == 0, jnp.cos(angles), -jnp.sin(angles)) * math.sqrt(2.0 / NLON)
    return values.astype(jnp.bfloat16)

def lat_weights(lat_rows):
    return jnp.cos(math.pi * ((lat_rows.astype(jnp.float32) + 0.5) / NLAT - 0.5))

def degrees(low_wave):
    columns = jnp.arange(NT + 2, dtype=jnp.int32)
    in_second = columns[None, :] >= NT + 1 - low_wave[:, None]
    degree = jnp.where(in_second, columns[None, :] - 1, low_wave[:, None] + columns[None, :])
    return (degree.astype(jnp.float32), in_second)

def reference(increment, background, legendre, coupling, damping, target_mass, numerators, pair_low, lat_map):
    fourier_tab = wave_table(pair_low)
    row_weight = lat_weights(lat_map)
    fourier = jnp.dot(fourier_tab, increment.reshape(LEV * NLAT, NLON).T, preferred_element_type=jnp.float32)
    fourier = (fourier.reshape(NPAIR, 4, LEV, NLAT) * row_weight).astype(jnp.bfloat16)
    degree, in_second = degrees(pair_low)

    def direct(packed):
        block_in, poly_tab, second = packed
        stored = poly_tab[lat_map]
        coeffs = jnp.dot(block_in.reshape(4 * LEV, NLAT), stored, preferred_element_type=jnp.float32)
        coeffs = coeffs.reshape(2, 2, LEV, NT + 2) * math.sqrt(2.0 / NLAT)
        return jnp.where(second, coeffs[1], coeffs[0])
    smoothing = 1.0 / (1.0 + (degree / NT) ** 4)
    incr_spec = lax.map(direct, (fourier, legendre, in_second)) * smoothing[:, None, None, :]
    shape_term = degree * (degree + 1.0) / (NT * (NT + 1.0))
    holder = (pair_low == 0).astype(jnp.float32)
    level_weight = 1.0 + 2.0 * jnp.arange(LEV, dtype=jnp.float32) / (LEV - 1)
    normaliser = jnp.sum(level_weight) * jnp.sum(lat_weights(jnp.arange(NLAT, dtype=jnp.int32))) * NLON
    fix_scale = math.sqrt(NT * NLON) / 2.0

    def inverse(packed):
        coeffs, poly_tab, second = packed
        stored = poly_tab[lat_map]
        zeros_bf = jnp.zeros_like(coeffs)
        split_rows = jnp.stack([jnp.where(second, zeros_bf, coeffs), jnp.where(second, coeffs, zeros_bf)])
        result = jnp.dot(split_rows.reshape(4 * LEV, NT + 2), stored.T, preferred_element_type=jnp.float32)
        return (result * math.sqrt(2.0 / NT)).astype(jnp.bfloat16).reshape(4, LEV, NLAT)
    spectral = background
    fix_list = []
    grid_now = jnp.zeros((LEV, NLAT, NLON), jnp.float32)
    for step_idx in range(STEPS):
        coupled = 0.7 * spectral + 0.4 * jnp.einsum('lm,prmc->prlc', coupling[step_idx], spectral, precision=lax.Precision.HIGHEST)
        weight_now = numerators[step_idx].astype(jnp.float32) / DEN
        spectral = coupled / (1.0 + damping[step_idx] * shape_term)[:, None, None, :] + weight_now * incr_spec
        waves = lax.map(inverse, (spectral.astype(jnp.bfloat16), legendre, in_second))
        grid_now = jnp.dot(waves.reshape(NPAIR * 4, LEV * NLAT).T, fourier_tab, preferred_element_type=jnp.float32).reshape(LEV, NLAT, NLON)
        total_mass = jnp.sum(jnp.exp(grid_now) * level_weight[:, None, None] * row_weight[None, :, None]) / normaliser
        mass_fix = jnp.log(target_mass[0] / total_mass)
        spectral = spectral.at[:, 0, :, 0].add(holder[:, None] * (mass_fix * fix_scale))
        fix_list.append(mass_fix)
    return (grid_now.astype(jnp.bfloat16), jnp.stack(fix_list))
```

```python
import math

import jax
import jax.numpy as jnp
import numpy as np
from jax import lax
from jax.sharding import PartitionSpec as P

NT = 767
NLAT = 768
NLON = 1536
LEV = 32
STEPS = 4
DEN = 64
NPAIR = 384
ALL = ("band", "lev")


def canonical_table():
    a = np.arange(NPAIR)[None, :]
    q = np.arange(2)[:, None]
    m = np.where(q == 0, a, NT - a)
    k = np.arange(NLON)
    t = (m[:, :, None] * k % NLON) * (2.0 * math.pi / NLON)
    tab = np.stack([np.cos(t), -np.sin(t)], axis=1) * math.sqrt(2.0 / NLON)
    return tab.astype(np.float32).astype(jnp.bfloat16)


def lat_weights(lat_rows):
    return jnp.cos(math.pi * ((lat_rows.astype(jnp.float32) + 0.5) / NLAT - 0.5))


def body(increment, background, legendre, coupling, damping, target_mass, numerators, pair_low, lat_map):
    nb, nv = lax.axis_size("band"), lax.axis_size("lev")
    band_id, lev_id = lax.axis_index("band"), lax.axis_index("lev")
    lev_dev, lat_dev, _ = increment.shape
    pair_dev = legendre.shape[0]
    onehot = (pair_low[:, None] == jnp.arange(NPAIR)[None, :]).astype(jnp.bfloat16)
    table = jnp.einsum("pa,qrak->pqrk", onehot, jnp.asarray(canonical_table()))
    table = table.reshape(NPAIR * 4, NLON).astype(jnp.bfloat16)
    local_lats = lax.dynamic_slice_in_dim(lat_map, band_id * lat_dev, lat_dev)
    row_weight = lat_weights(local_lats)
    level_weight = 1.0 + 2.0 * jnp.arange(LEV, dtype=jnp.float32) / (LEV - 1)
    normaliser = jnp.sum(level_weight) * jnp.sum(lat_weights(jnp.arange(NLAT))) * NLON
    own = lax.dynamic_slice_in_dim(pair_low, (band_id * nv + lev_id) * pair_dev, pair_dev)
    cols = jnp.arange(NT + 2)
    second = cols[None, :] >= NT + 1 - own[:, None]
    degree = jnp.where(second, cols[None, :] - 1, own[:, None] + cols[None, :]).astype(jnp.float32)
    perm = (lat_map[:, None] == jnp.arange(NLAT)[None, :]).astype(jnp.bfloat16)
    stored = jnp.einsum("sj,pjc->psc", perm, legendre, preferred_element_type=jnp.float32).astype(jnp.bfloat16)
    fourier = jnp.einsum("ck,xk->cx", table, increment.reshape(lev_dev * lat_dev, NLON), preferred_element_type=jnp.float32)
    fourier = (fourier.reshape(NPAIR, 4, lev_dev, lat_dev) * row_weight).astype(jnp.bfloat16)
    got = lax.all_to_all(fourier, ALL, split_axis=0, concat_axis=0, tiled=True)
    got = got.reshape(nb, nv, pair_dev, 4, lev_dev, lat_dev).transpose(2, 3, 1, 4, 0, 5).reshape(pair_dev, 4 * LEV, NLAT)
    coeffs = jnp.einsum("prj,pjc->prc", got, stored, preferred_element_type=jnp.float32)
    coeffs = coeffs.reshape(pair_dev, 2, 2, LEV, NT + 2) * math.sqrt(2.0 / NLAT)
    sec = second[:, None, None, :]
    incr = jnp.where(sec, coeffs[:, 1], coeffs[:, 0]) * (1.0 / (1.0 + (degree / NT) ** 4))[:, None, None, :]
    shape_term = degree * (degree + 1.0) / (NT * (NT + 1.0))
    spectral = background
    states = []
    for s in range(STEPS):
        coupled = 0.7 * spectral + 0.4 * jnp.einsum("lm,prmc->prlc", coupling[s], spectral, precision=lax.Precision.HIGHEST)
        spectral = coupled / (1.0 + damping[s] * shape_term)[:, None, None, :] + numerators[s].astype(jnp.float32) / DEN * incr
        states.append(spectral.astype(jnp.bfloat16))
    st = jnp.stack(states, axis=1)
    zero = jnp.zeros_like(st)
    sec = sec[:, None]
    split = jnp.stack([jnp.where(sec, zero, st), jnp.where(sec, st, zero)], axis=2)
    waves = jnp.einsum("pxc,pjc->pxj", split.reshape(pair_dev, STEPS * 4 * LEV, NT + 2), stored, preferred_element_type=jnp.float32)
    waves = (waves * math.sqrt(2.0 / NT)).astype(jnp.bfloat16)
    waves = waves.reshape(pair_dev, STEPS, 4, nv, lev_dev, nb, lat_dev).transpose(5, 3, 0, 2, 1, 4, 6)
    back = lax.all_to_all(waves.reshape(nb * nv, pair_dev * 4, STEPS * lev_dev * lat_dev), ALL, split_axis=0, concat_axis=0, tiled=True)
    grid = jnp.einsum("cx,ck->xk", back.reshape(NPAIR * 4, STEPS * lev_dev * lat_dev), table, preferred_element_type=jnp.float32)
    grid = grid.reshape(STEPS, lev_dev, lat_dev, NLON)
    top = jnp.max(grid, axis=(2, 3))
    mass = jnp.sum(jnp.sum(jnp.exp(grid - top[:, :, None, None]), axis=3) * row_weight, axis=2)
    tops = lax.all_gather(top, ALL).reshape(nb, nv, STEPS, lev_dev).transpose(0, 2, 1, 3).reshape(nb, STEPS, LEV)
    masses = lax.all_gather(mass, ALL).reshape(nb, nv, STEPS, lev_dev).transpose(0, 2, 1, 3).reshape(nb, STEPS, LEV)
    to_grid = math.sqrt(2.0 / NT) * float(np.float32(math.sqrt(2.0 / NLON)).astype(jnp.bfloat16))
    delta = jnp.zeros((LEV,), jnp.float32)
    fixes = []
    for s in range(STEPS):
        delta = 0.7 * delta + 0.4 * jnp.dot(coupling[s], delta, precision=lax.Precision.HIGHEST)
        shift = delta * to_grid
        total = jnp.sum(jnp.exp(tops[:, s] + shift) * masses[:, s] * level_weight) / normaliser
        fix = jnp.log(target_mass[0] / total)
        fixes.append(fix)
        if s < STEPS - 1:
            delta = delta + fix * (math.sqrt(NT * NLON) / 2.0)
    mine = lax.dynamic_slice_in_dim(shift, lev_id * lev_dev, lev_dev)
    out = (grid[STEPS - 1] + mine[:, None, None]).astype(jnp.bfloat16)
    return out, jnp.stack(fixes)


def solution(mesh):
    placed = (P("lev", "band", None), P(ALL, None, None, None), P(ALL, None, None), P(), P(), P(), P(), P(), P())
    return jax.shard_map(body, mesh=mesh, in_specs=placed, out_specs=(P("lev", "band", None), P()), check_vma=False)
```
